32 devices in a mesh: section: 4 (over z), dp: 8 (over y, x, core).
Axes of the slice: x: 2, y: 2, z: 4, core: 2. Of those that a mesh axis runs over, the one named last changes fastest.
Arguments:
- stream: float32 [2, 64, 16, 16, 128], P(None, 'dp'), may hold values from -6 to 6
- cotangent: float32 [2, 64, 16, 16, 128], P(None, 'dp'), may hold values from -6 to 6
- weights: bfloat16 [4, 2304, 128], P('section'), may hold values from -0.09375 to 0.09375
- master: float32 [4, 2304, 128], P('section', 'dp'), may hold values from -0.09375 to 0.09375
- momentum: float32 [4, 2304, 128], P('section', 'dp'), may hold values from -6 to 6
Outputs:
- new_master: float32 [4, 2304, 128], P('section', 'dp')
- new_momentum: float32 [4, 2304, 128], P('section', 'dp')
- new_weights: bfloat16 [4, 2304, 128], P('section')
The draws below stay inside these ranges and needn't reach their ends.
All inputs are finite; a program needn't handle non-finite values.
Results may differ from the reference program's by a relative error of at most 0.014.
Values may be sent and summed in bfloat16 or wider, within the bound.
A program may use at most 64 MiB of HBM per device.

```python
import jax
import jax.numpy as jnp
from jax import lax

C = 128
SIDE = 16
LAYERS = 1
SECTIONS = 4
IMAGES = 64
ROWS = 2304
N_SECTION = 4


def block_levels(own_key, shape, cuts, least, largest):
    loudness, own = 1.0, jax.random.fold_in(own_key, 6)
    for dim, parts in cuts:
        heights = jnp.exp(jax.random.uniform(jax.random.fold_in(own, dim), (parts,), jnp.float32, least / len(cuts), largest / len(cuts)))
        loudness = loudness * jnp.repeat(heights, shape[dim] // parts).reshape([-1 if axis == dim else 1 for axis in range(len(shape))])
    return loudness


def scatter_about(key, extent, scale, most, split=(), held_as=jnp.bfloat16):
    level = block_levels(key, extent, split, -0.22, 0.18) if split else 1.0
    entries = jax.random.normal(key, extent, jnp.float32) * scale * level
    return jnp.minimum(jnp.maximum(entries, -most), most).astype(held_as)


def setup_inputs(seed: int = 0) -> dict:
    seeds = jax.random.split(jax.random.key(seed), 6)
    stream = scatter_about(seeds[0], (2, IMAGES, SIDE, SIDE, C), 1.0, 6.0, ((1, 8),), jnp.float32)
    cotangent = scatter_about(seeds[1], (2, IMAGES, SIDE, SIDE, C), 1.0, 6.0, ((1, 8),), jnp.float32)
    weights = scatter_about(seeds[2], (SECTIONS, ROWS, C), (36 * C) ** -0.5, 0.09375, ((0, 4),))
    master = scatter_about(seeds[3], (SECTIONS, ROWS, C), (36 * C) ** -0.5, 0.09375, ((0, 4), (1, 8)), jnp.float32)
    momentum = scatter_about(seeds[4], (SECTIONS, ROWS, C), 1.0, 6.0, ((0, 4), (1, 8)), jnp.float32)
    return dict(stream=stream, cotangent=cotangent, weights=weights, master=master, momentum=momentum)


step_size = 0.1
inertia = 0.9

def product(left_op, right_op, dims):
    return lax.dot_general(left_op.astype(jnp.float32), right_op.astype(jnp.float32), (dims, ((), ())), precision=lax.Precision.HIGHEST, preferred_element_type=jnp.float32)

def columns(field):
    height = field.shape[1]
    breadth = field.shape[2]
    padded = jnp.pad(jax.nn.silu(field).astype(jnp.bfloat16), ((0, 0), (1, 1), (1, 1), (0, 0)))
    shifted = [padded[:, row_tap:row_tap + height, col_tap:col_tap + breadth, :] for row_tap in range(3) for col_tap in range(3)]
    return jnp.concatenate(shifted, axis=3).reshape(-1, 9 * field.shape[3])

def convolve(patches, weight, template):
    return product(patches, weight, ((1,), (0,))).reshape(template.shape)

def spread(rounded, weight, template):
    height, breadth, channels = (template.shape[1], template.shape[2], template.shape[3])
    spread_cols = product(rounded, weight, ((1,), (1,))).reshape(template.shape[0], height, breadth, 9 * channels)
    padded = jnp.pad(spread_cols, ((0, 0), (1, 1), (1, 1), (0, 0)))
    summed = jnp.zeros(template.shape, jnp.float32)
    for row_tap in range(3):
        for col_tap in range(3):
            tap_index = 3 * row_tap + col_tap
            summed = summed + padded[:, 2 - row_tap:2 - row_tap + height, 2 - col_tap:2 - col_tap + breadth, tap_index * channels:(tap_index + 1) * channels]
    return summed

def weight_grad(patches, rounded):
    return product(patches, rounded, ((0,), (0,)))

def silu_slope(field):
    logistic = jax.nn.sigmoid(field)
    return logistic * (1.0 + field * (1.0 - logistic))

def coupling_forward(first, second, weight_f, weight_g):
    patch_f = columns(second)
    out_first = first + convolve(patch_f, weight_f, second)
    patch_g = columns(out_first)
    out_second = second + convolve(patch_g, weight_g, out_first)
    return (out_first, out_second)

def coupling_backward(out_first, out_second, grad_first, grad_second, weight_f, weight_g):
    channels = out_first.shape[3]
    patch_g = columns(out_first)
    second = out_second - convolve(patch_g, weight_g, out_first)
    patch_f = columns(second)
    first = out_first - convolve(patch_f, weight_f, second)
    round_second = grad_second.astype(jnp.bfloat16).reshape(-1, channels)
    wgrad_g = weight_grad(patch_g, round_second)
    grad_first = grad_first + spread(round_second, weight_g, out_first) * silu_slope(out_first)
    round_first = grad_first.astype(jnp.bfloat16).reshape(-1, channels)
    wgrad_f = weight_grad(patch_f, round_first)
    grad_second = grad_second + spread(round_first, weight_f, second) * silu_slope(second)
    return (first, second, grad_first, grad_second, wgrad_f, wgrad_g)

def reference(stream, cotangent, weights, master, momentum):
    blocks = weights.reshape(N_SECTION, LAYERS, 2, 9 * C, C)
    first, second = (stream[0], stream[1])
    for section_idx in range(N_SECTION):
        for coupling in range(LAYERS):
            first, second = coupling_forward(first, second, blocks[section_idx, coupling, 0], blocks[section_idx, coupling, 1])
    grad_first, grad_second = (cotangent[0], cotangent[1])
    section_grads = []
    for section_idx in reversed(range(N_SECTION)):
        pieces = []
        for coupling in reversed(range(LAYERS)):
            first, second, grad_first, grad_second, wgrad_f, wgrad_g = coupling_backward(first, second, grad_first, grad_second, blocks[section_idx, coupling, 0], blocks[section_idx, coupling, 1])
            pieces.append(jnp.stack([wgrad_f, wgrad_g]))
        pieces = pieces[::-1]
        section_grads.append(jnp.stack(pieces).reshape(LAYERS * 18 * C, C))
    section_grads = section_grads[::-1]
    gradient = jnp.stack(section_grads) / IMAGES
    new_momentum = inertia * momentum + gradient
    new_master = master - step_size * new_momentum
    return (new_master, new_momentum, new_master.astype(jnp.bfloat16))
```

```python
import functools
import math

import jax
import jax.numpy as jnp
from jax import lax
from jax.experimental import pallas as pl
from jax.experimental.pallas import tpu as pltpu
from jax.sharding import PartitionSpec as P

MESH = pl.DeviceIdType.MESH
step_size = 0.1
inertia = 0.9


def kernel(
    S, D, images,
    stream, cotangent, weights, master, momentum,
    new_master, new_momentum, new_weights,
    wbuf, xs, ds, pads, kept, slopes, g32, gsend, pairs, recv1, zsend, recv2, gown, spread_out, old_master, old_momentum,
    in_sem, own_sem, w1send, w1recv, w2send, w2recv, w3send, w3recv,
    psend, precv, gsend_sem, grecv_sem, zsend_sem, zrecv_sem,
    osend_sem, orecv_sem, fsend_sem, frecv_sem,
):
    s = lax.axis_index("section")
    d = lax.axis_index("dp")
    core = lax.rem(d, 2)
    partner = d + 1 - 2 * core
    chips = D // 2
    share, H, W, C = xs.shape[1:]
    M = share * H * W
    rows = master.shape[0]
    R = rows * D
    NC = math.gcd(R // 16, D)
    part = R // NC

    def chunk(i):
        return pl.ds(pl.multiple_of(i * part, 16), part)

    def other_chip(i):
        return lax.rem(d + 2 * i, D)

    def section_copy(src, to):
        return pltpu.make_async_remote_copy(
            src_ref=weights.at[chunk(d)], dst_ref=wbuf.at[src, chunk(d)],
            send_sem=w1send.at[to], recv_sem=w1recv.at[src],
            device_id=(to, d), device_id_type=MESH)

    def layer_copy(sec, src, to):
        return pltpu.make_async_remote_copy(
            src_ref=wbuf.at[sec, chunk(src)], dst_ref=wbuf.at[sec, chunk(src)],
            send_sem=w2send.at[sec, to], recv_sem=w2recv.at[sec, src],
            device_id=(s, to), device_id_type=MESH)

    def core_copy(sec, src):
        return pltpu.make_async_remote_copy(
            src_ref=wbuf.at[sec, chunk(src)], dst_ref=wbuf.at[sec, chunk(src)],
            send_sem=w3send.at[sec, src], recv_sem=w3recv.at[sec, src],
            device_id=(s, partner), device_id_type=MESH)

    barrier = pltpu.get_barrier_semaphore()

    @pl.loop(1, S)
    def _(i):
        pl.semaphore_signal(barrier, inc=1, device_id=(lax.rem(s + i, S), d), device_id_type=MESH)

    @pl.loop(1, D)
    def _(i):
        pl.semaphore_signal(barrier, inc=1, device_id=(s, lax.rem(d + i, D)), device_id_type=MESH)

    load_own = pltpu.make_async_copy(weights, wbuf.at[s], own_sem)
    load_own.start()
    mine = pl.ds(s * share, share)
    loads = [
        pltpu.make_async_copy(stream.at[0, mine], xs.at[0], in_sem.at[0]),
        pltpu.make_async_copy(stream.at[1, mine], xs.at[1], in_sem.at[1]),
        pltpu.make_async_copy(cotangent.at[0, mine], ds.at[0], in_sem.at[2]),
        pltpu.make_async_copy(cotangent.at[1, mine], ds.at[1], in_sem.at[3]),
    ]
    for load in loads:
        load.start()
    states = [
        pltpu.make_async_copy(momentum, old_momentum, in_sem.at[4]),
        pltpu.make_async_copy(master, old_master, in_sem.at[5]),
    ]
    for load in states:
        load.start()
    with jax.named_scope("t_bar"):
        pl.semaphore_wait(barrier, S + D - 2)

    @pl.when(d < NC)
    def _():
        for i in range(1, S):
            section_copy(s, lax.rem(s + i, S)).start()

    zero_row = jnp.zeros((share, 1, W, 3 * C), jnp.bfloat16)
    for k in range(2):
        pads[k, :, 0:1] = zero_row
        pads[k, :, H + 1 : H + 2] = zero_row

    col = lax.rem(lax.broadcasted_iota(jnp.int32, (M, C), 0), W)

    def shifted(k, flat, order):
        before = jnp.where(col == 0, 0.0, pltpu.roll(flat, 1, 0))
        after = jnp.where(col == W - 1, 0.0, pltpu.roll(flat, M - 1, 0))
        for b, piece in enumerate((before, flat, after) if order else (after, flat, before)):
            pads[k, :, 1 : H + 1, :, b * C : (b + 1) * C] = piece.astype(jnp.bfloat16).reshape(
                share, H, W, C)

    def activate(value, sec, which):
        logistic = 1.0 / (1.0 + jnp.exp(-value))
        act = value * logistic
        slopes[sec, which] = logistic * (1.0 + value * (1.0 - logistic))
        kept[sec, which] = act.astype(jnp.bfloat16)
        shifted(0, act, True)

    def conv(sec, which):
        total = jnp.zeros((M, C), jnp.float32)
        for a in range(3):
            total += jnp.dot(
                pads[0, :, a : a + H].reshape(M, 3 * C),
                wbuf[sec, which * 9 * C + a * 3 * C : which * 9 * C + (a + 1) * 3 * C],
                preferred_element_type=jnp.float32)
        return total

    def relay(sec):
        @pl.when((sec != s) & (d < NC))
        def _():
            section_copy(sec, s).wait_recv()
            layer_copy(sec, d, partner).start()

            @pl.loop(1, chips)
            def _(i):
                layer_copy(sec, d, other_chip(i)).start()

    def pass_on(sec):
        @pl.when(sec != s)
        def _():
            @pl.loop(1, chips)
            def _(i):
                src = other_chip(i)

                @pl.when(src < NC)
                def _():
                    layer_copy(sec, src, d).wait_recv()
                    core_copy(sec, src).start()

    def take(sec):
        @pl.when(sec != s)
        def _():
            @pl.when(partner < NC)
            def _():
                layer_copy(sec, partner, d).wait_recv()

            @pl.loop(1, chips)
            def _(i):
                src = lax.rem(partner + 2 * i, D)

                @pl.when(src < NC)
                def _():
                    core_copy(sec, src).wait_recv()

    with jax.named_scope("t_start"):
        load_own.wait()
        for load in loads:
            load.wait()
        for sec in range(S):
            relay(sec)
        pass_on(0)

    def forward_one(sec, carry):
        first = xs[0].reshape(M, C)
        second = xs[1].reshape(M, C)
        with jax.named_scope("t_act_take"):
            activate(second, sec, 0)
            take(sec)
        with jax.named_scope("t_conv0"):
            first = first + conv(sec, 0)
        with jax.named_scope("t_act1"):
            activate(first, sec, 1)
        xs[0] = first.reshape(share, H, W, C)

        @pl.when(sec + 1 < S)
        def _():
            pass_on(sec + 1)

        with jax.named_scope("t_conv1"):
            xs[1] = (second + conv(sec, 1)).reshape(share, H, W, C)
        return carry

    lax.fori_loop(0, S, forward_one, 0)

    def pair_copy(sec, to):
        return pltpu.make_async_remote_copy(
            src_ref=gsend.at[sec, to], dst_ref=pairs.at[sec, to],
            send_sem=psend.at[sec, to], recv_sem=precv.at[sec, to],
            device_id=(s, partner), device_id_type=MESH)

    def grad_copy(sec, src, to):
        return pltpu.make_async_remote_copy(
            src_ref=gsend.at[sec, to], dst_ref=recv1.at[sec, src],
            send_sem=gsend_sem.at[sec, to], recv_sem=grecv_sem.at[sec, src],
            device_id=(s, to), device_id_type=MESH)

    def sum_copy(sec, src):
        return pltpu.make_async_remote_copy(
            src_ref=zsend.at[sec], dst_ref=recv2.at[src],
            send_sem=zsend_sem.at[sec], recv_sem=zrecv_sem.at[src],
            device_id=(sec, d), device_id_type=MESH)

    def grads(sec, which):
        with jax.named_scope("t_wgrad"):
            rounded = ds[1 if which else 0].reshape(M, C)
            shifted(1, rounded, False)
            act = kept[sec, which]
            for a in range(3):
                block = lax.dot_general(
                    act, pads[1, :, 2 - a : 2 - a + H].reshape(M, 3 * C),
                    (((0,), (0,)), ((), ())), preferred_element_type=jnp.float32)
                for b in range(3):
                    g32[(3 * a + b) * C : (3 * a + b + 1) * C] = block[:, b * C : (b + 1) * C]
        per = D // 2

        def convert(at):
            gsend[sec, which * per + at] = g32[
                pl.ds(pl.multiple_of(at * rows, 8), rows)].astype(jnp.bfloat16)

        with jax.named_scope("t_convert"):
            @pl.loop(0, per // 2)
            def _(i):
                at = 2 * i + 1 - core
                convert(at)
                pair_copy(sec, which * per + at).start()

            @pl.loop(0, per // 2)
            def _(i):
                convert(2 * i + core)

        with jax.named_scope("t_dgrad"):
            total = jnp.zeros((M, C), jnp.float32)
            for a in range(3):
                for b in range(3):
                    tap = 3 * a + b
                    total += lax.dot_general(
                        pads[1, :, 2 - a : 2 - a + H, :, b * C : (b + 1) * C].reshape(M, C),
                        wbuf[sec, which * 9 * C + tap * C : which * 9 * C + (tap + 1) * C],
                        (((1,), (1,)), ((), ())), preferred_element_type=jnp.float32)
            into = 0 if which else 1
            ds[into] = ds[into] + (total * slopes[sec, which]).reshape(share, H, W, C)

    def combine(sec, which):
        per = D // 2

        @pl.loop(0, per // 2)
        def _(i):
            to = which * per + 2 * i + core
            pair_copy(sec, to).wait_recv()
            both = gsend[sec, to].astype(jnp.float32) + pairs[sec, to].astype(jnp.float32)
            gsend[sec, to] = both.astype(jnp.bfloat16)

            @pl.when(to != d)
            def _():
                grad_copy(sec, d, to).start()

    def finish(sec):
        def add(i, total):
            src = other_chip(i)
            grad_copy(sec, src, d).wait_recv()
            return total + recv1[sec, src].astype(jnp.float32)

        total = lax.fori_loop(1, chips, add, gsend[sec, d].astype(jnp.float32))

        @pl.when(sec == s)
        def _():
            gown[...] = total

        @pl.when(sec != s)
        def _():
            zsend[sec] = total.astype(jnp.bfloat16)
            sum_copy(sec, s).start()

    def backward_one(turn, carry):
        sec = S - 1 - turn
        grads(sec, 1)
        with jax.named_scope("t_comb1"):
            combine(sec, 1)

        with jax.named_scope("t_fin"):
            @pl.when(turn > 0)
            def _():
                finish(sec + 1)

        grads(sec, 0)
        with jax.named_scope("t_comb0"):
            combine(sec, 0)
        return carry

    lax.fori_loop(0, S, backward_one, 0)
    with jax.named_scope("t_finish0"):
        finish(0)

    def gather_sums(i, total):
        src = lax.rem(s + i, S)
        sum_copy(s, src).wait_recv()
        return total + recv2[src].astype(jnp.float32)

    with jax.named_scope("t_sum"):
        summed = lax.fori_loop(1, S, gather_sums, gown[...])
        for load in states:
            load.wait()
        moved = inertia * old_momentum[...] + summed / images
        new_momentum[...] = moved
        fresh = old_master[...] - step_size * moved
        new_master[...] = fresh
        spread_out[d] = fresh.astype(jnp.bfloat16)

    def out_copy(src, to):
        return pltpu.make_async_remote_copy(
            src_ref=spread_out.at[src], dst_ref=spread_out.at[src],
            send_sem=osend_sem.at[to], recv_sem=orecv_sem.at[src],
            device_id=(s, to), device_id_type=MESH)

    def hand_over(src):
        return pltpu.make_async_remote_copy(
            src_ref=spread_out.at[src], dst_ref=spread_out.at[src],
            send_sem=fsend_sem.at[src], recv_sem=frecv_sem.at[src],
            device_id=(s, partner), device_id_type=MESH)

    with jax.named_scope("t_out"):
        @pl.loop(1, chips)
        def _(i):
            out_copy(d, other_chip(i)).start()

        out_copy(d, partner).start()

        @pl.loop(1, S)
        def _(i):
            other = lax.rem(s + i, S)
            sum_copy(other, s).wait_send()

            @pl.when(d < NC)
            def _():
                section_copy(s, other).wait_send()
                layer_copy(other, d, partner).wait_send()

            @pl.loop(1, chips)
            def _(j):
                @pl.when(d < NC)
                def _():
                    layer_copy(other, d, other_chip(j)).wait_send()

                @pl.when(other_chip(j) < NC)
                def _():
                    core_copy(other, other_chip(j)).wait_send()

        @pl.loop(0, S)
        def _(sec):
            @pl.loop(1, chips)
            def _(i):
                grad_copy(sec, d, other_chip(i)).wait_send()

            @pl.loop(0, chips)
            def _(i):
                pair_copy(sec, 2 * i + 1 - core).wait_send()

        @pl.loop(1, chips)
        def _(i):
            src = other_chip(i)
            out_copy(src, d).wait_recv()
            hand_over(src).start()

        out_copy(partner, d).wait_recv()
        out_copy(d, partner).wait_send()

        @pl.loop(1, chips)
        def _(i):
            out_copy(d, other_chip(i)).wait_send()
            hand_over(other_chip(i)).wait_send()
            hand_over(lax.rem(partner + 2 * i, D)).wait_recv()

        new_weights[...] = spread_out[...]


def store(a, b, c, out_a, out_b, out_c, sem):
    copies = [
        pltpu.make_async_copy(c, out_c, sem.at[2]),
        pltpu.make_async_copy(a, out_a, sem.at[0]),
        pltpu.make_async_copy(b, out_b, sem.at[1]),
    ]
    for copy in copies:
        copy.start()
    for copy in copies:
        copy.wait()


def on_device(S, D, stream, cotangent, weights, master, momentum):
    _, per_dp, H, W, C = stream.shape
    share = per_dp // S
    M = share * H * W
    R = weights.shape[1]
    rows = master.shape[1]
    bf, f32 = jnp.bfloat16, jnp.float32
    vmem = pl.BlockSpec(memory_space=pltpu.VMEM)
    hbm = pl.BlockSpec(memory_space=pltpu.HBM)
    dma = pltpu.SemaphoreType.DMA
    results = pl.pallas_call(
        functools.partial(kernel, S, D, per_dp * D),
        out_shape=(
            pltpu.VMEM((rows, C), f32),
            pltpu.VMEM((rows, C), f32),
            pltpu.VMEM((D, rows, C), bf),
        ),
        in_specs=[hbm] * 5,
        out_specs=(vmem, vmem, vmem),
        scratch_shapes=[
            pltpu.VMEM((S, R, C), bf),
            pltpu.VMEM((2, share, H, W, C), f32),
            pltpu.VMEM((2, share, H, W, C), f32),
            pltpu.VMEM((2, share, H + 2, W, 3 * C), bf),
            pltpu.VMEM((S, 2, M, C), bf),
            pltpu.VMEM((S, 2, M, C), f32),
            pltpu.VMEM((R // 2, C), f32),
            pltpu.VMEM((S, D, rows, C), bf),
            pltpu.VMEM((S, D, rows, C), bf),
            pltpu.VMEM((S, D, rows, C), bf),
            pltpu.VMEM((S, rows, C), bf),
            pltpu.VMEM((S, rows, C), bf),
            pltpu.VMEM((rows, C), f32),
            pltpu.VMEM((D, rows, C), bf),
            pltpu.VMEM((rows, C), f32),
            pltpu.VMEM((rows, C), f32),
            dma((6,)), dma, dma((S,)), dma((S,)), dma((S, D)), dma((S, D)), dma((S, D)), dma((S, D)),
            dma((S, D)), dma((S, D)), dma((S, D)), dma((S, D)), dma((S,)), dma((S,)),
            dma((D,)), dma((D,)), dma((D,)), dma((D,)),
        ],
        compiler_params=pltpu.CompilerParams(
            has_side_effects=True, collective_id=0, vmem_limit_bytes=48 * 1024 * 1024),
    )(*[pltpu.with_memory_space_constraint(x, pltpu.HBM)
        for x in (stream, cotangent, weights[0], master[0], momentum[0])])
    new_master, new_momentum, new_weights = pl.pallas_call(
        store,
        out_shape=(
            jax.ShapeDtypeStruct((rows, C), f32),
            jax.ShapeDtypeStruct((rows, C), f32),
            jax.ShapeDtypeStruct((D, rows, C), bf),
        ),
        in_specs=[vmem] * 3,
        out_specs=(hbm, hbm, hbm),
        scratch_shapes=[dma((3,))],
        compiler_params=pltpu.CompilerParams(vmem_limit_bytes=4 * 1024 * 1024),
    )(*[pltpu.with_memory_space_constraint(x, pltpu.VMEM) for x in results])
    return (new_master[None], new_momentum[None], new_weights.reshape(1, R, C))


def solution(mesh):
    placed = (
        P(None, "dp", None, None, None),
        P(None, "dp", None, None, None),
        P("section", None, None),
        P("section", "dp", None),
        P("section", "dp", None),
    )
    return jax.shard_map(
        functools.partial(on_device, mesh.shape["section"], mesh.shape["dp"]),
        mesh=mesh,
        in_specs=placed,
        out_specs=(P("section", "dp", None), P("section", "dp", None), P("section", None, None)),
        check_vma=False,
    )
```

```python
import functools
import math

import jax
import jax.numpy as jnp
from jax import lax
from jax.experimental import pallas as pl
from jax.experimental.pallas import tpu as pltpu
from jax.sharding import PartitionSpec as P

MESH = pl.DeviceIdType.MESH
step_size = 0.1
inertia = 0.9
scope = jax.named_scope


def kernel(
    S, D, images, NP,
    stream, cotangent, weights, master, momentum,
    new_master, new_momentum, new_weights,
    wbuf, xs, ds, pads, kept, slopes, g32, gsend, pairs, recv1, zsend, recv2, gown,
    old_master, old_momentum,
    in_sem, zs, zr, ls, lr, cs, cr, ps, pr, gs, gr, us, ur, os, orr, fs, fr,
):
    s = lax.axis_index("section")
    d = lax.axis_index("dp")
    core = lax.rem(d, 2)
    chip = lax.div(d, 2)
    partner = d + 1 - 2 * core
    chips = D // 2
    HC = chips // 2
    share, H, W, C = xs.shape[1:]
    M = share * H * W
    rows = master.shape[0]
    sub = rows // NP
    R = rows * D
    half = R // 2
    NC = math.gcd(half // 16, D)
    CK = NC // 2
    piece = half // NC
    sends = chip < CK

    def other_chip(i):
        return lax.rem(chip + i, chips)

    def own_piece(h):
        return pl.ds(pl.multiple_of(h * half + (core * CK + chip) * piece, 16), piece)

    def section_copy(sec, h, to):
        return pltpu.make_async_remote_copy(
            src_ref=weights.at[own_piece(h)], dst_ref=wbuf.at[sec, own_piece(h)],
            send_sem=zs, recv_sem=zr.at[sec, h],
            device_id=(to, d), device_id_type=MESH)

    def layer_copy(sec, h, to):
        return pltpu.make_async_remote_copy(
            src_ref=wbuf.at[sec, own_piece(h)], dst_ref=wbuf.at[sec, own_piece(h)],
            send_sem=ls.at[sec, h], recv_sem=lr.at[sec, h],
            device_id=(s, 2 * to + core), device_id_type=MESH)

    def core_copy(sec, h):
        at = pl.ds(pl.multiple_of(h * half + core * (CK * piece), 16), CK * piece)
        return pltpu.make_async_remote_copy(
            src_ref=wbuf.at[sec, at], dst_ref=wbuf.at[sec, at],
            send_sem=cs.at[sec], recv_sem=cr.at[sec, h],
            device_id=(s, partner), device_id_type=MESH)

    def all_of(ref, send_sem, recv_sem):
        return pltpu.make_async_remote_copy(
            src_ref=ref, dst_ref=ref, send_sem=send_sem, recv_sem=recv_sem,
            device_id=(s, partner), device_id_type=MESH)

    def send_down():
        for h in range(2):
            for to in range(S - 1):
                @pl.when(sends & (to < s))
                def _():
                    section_copy(s, h, to).start()

    def send_up():
        for h in range(2):
            for to in range(S - 1, 0, -1):
                @pl.when(sends & (to > s))
                def _():
                    section_copy(s, h, to).start()

    def relay(sec, h):
        @pl.when((sec != s) & (sec < S) & sends)
        def _():
            section_copy(sec, h, s).wait_recv()

            @pl.loop(1, chips)
            def _(i):
                layer_copy(sec, h, other_chip(i)).start()

    def pass_on(sec, h):
        @pl.when((sec != s) & (sec < S))
        def _():
            @pl.when(sends)
            def _():
                all_of(wbuf.at[sec, pl.ds(0, (CK - 1) * piece)], ls.at[sec, h], lr.at[sec, h]).wait_recv()

            if CK < chips:
                @pl.when(chip >= CK)
                def _():
                    all_of(wbuf.at[sec, pl.ds(0, CK * piece)], ls.at[sec, h], lr.at[sec, h]).wait_recv()

            core_copy(sec, h).start()

    def take(sec, h):
        @pl.when(sec != s)
        def _():
            core_copy(sec, h).wait_recv()

    barrier = pltpu.get_barrier_semaphore()

    @pl.loop(1, S)
    def _(i):
        pl.semaphore_signal(barrier, inc=1, device_id=(lax.rem(s + i, S), d), device_id_type=MESH)

    @pl.loop(1, D)
    def _(i):
        pl.semaphore_signal(barrier, inc=1, device_id=(s, lax.rem(d + i, D)), device_id_type=MESH)

    mine = pl.ds(s * share, share)
    loads = [
        pltpu.make_async_copy(stream.at[1, mine], xs.at[1], in_sem.at[1]),
        pltpu.make_async_copy(stream.at[0, mine], xs.at[0], in_sem.at[0]),
        pltpu.make_async_copy(weights, wbuf.at[s], in_sem.at[6]),
        pltpu.make_async_copy(cotangent.at[0, mine], ds.at[0], in_sem.at[2]),
        pltpu.make_async_copy(cotangent.at[1, mine], ds.at[1], in_sem.at[3]),
        pltpu.make_async_copy(momentum, old_momentum, in_sem.at[4]),
        pltpu.make_async_copy(master, old_master, in_sem.at[5]),
    ]
    for load in loads:
        load.start()

    zero_row = jnp.zeros((share, 1, W, 3 * C), jnp.bfloat16)
    for k in range(2):
        pads[k, :, 0:1] = zero_row
        pads[k, :, H + 1 : H + 2] = zero_row

    with scope("t_bar"):
        pl.semaphore_wait(barrier, S + D - 2)
    send_down()

    @pl.when(s == 0)
    def _():
        send_up()

    col = lax.rem(lax.broadcasted_iota(jnp.int32, (M, C), 0), W)

    def shifted(k, flat, order):
        before = jnp.where(col == 0, 0.0, pltpu.roll(flat, 1, 0))
        after = jnp.where(col == W - 1, 0.0, pltpu.roll(flat, M - 1, 0))
        for b, piece_ in enumerate((before, flat, after) if order else (after, flat, before)):
            pads[k, :, 1 : H + 1, :, b * C : (b + 1) * C] = piece_.astype(jnp.bfloat16).reshape(
                share, H, W, C)

    def activate(value, sec, which):
        logistic = 1.0 / (1.0 + jnp.exp(-value))
        act = value * logistic
        slopes[sec, which] = logistic * (1.0 + value * (1.0 - logistic))
        kept[sec, which] = act.astype(jnp.bfloat16)
        shifted(0, act, True)

    def conv(sec, which):
        total = jnp.zeros((M, C), jnp.float32)
        for a in range(3):
            total += jnp.dot(
                pads[0, :, a : a + H].reshape(M, 3 * C),
                wbuf[sec, which * 9 * C + a * 3 * C : which * 9 * C + (a + 1) * 3 * C],
                preferred_element_type=jnp.float32)
        return total

    with scope("t_load"):
        for load in loads[:3]:
            load.wait()
    with scope("t_act"):
        activate(xs[1].reshape(M, C), 0, 0)
    with scope("t_rel"):
        relay(0, 0)

        @pl.when(s > 0)
        def _():
            send_up()

        relay(0, 1)
    with scope("t_pass"):
        pass_on(0, 0)

    def forward_one(sec, carry):
        with scope("t_rel"):
            relay(sec + 1, 0)
        with scope("t_take"):
            take(sec, 0)
        with scope("t_conv"):
            first = xs[0].reshape(M, C) + conv(sec, 0)
        with scope("t_act"):
            activate(first, sec, 1)
            xs[0] = first.reshape(share, H, W, C)
        with scope("t_pass"):
            pass_on(sec, 1)
        with scope("t_rel"):
            relay(sec + 1, 1)
        with scope("t_take"):
            take(sec, 1)
        with scope("t_conv"):
            second = xs[1].reshape(M, C) + conv(sec, 1)

        @pl.when(sec + 1 < S)
        def _():
            with scope("t_act"):
                activate(second, sec + 1, 0)
                xs[1] = second.reshape(share, H, W, C)
            with scope("t_pass"):
                pass_on(sec + 1, 0)

        return carry

    lax.fori_loop(0, S, forward_one, 0)
    for load in loads[3:]:
        load.wait()

    def pair_copy(sec, which):
        at = pl.ds(which * HC, HC)
        return pltpu.make_async_remote_copy(
            src_ref=gsend.at[sec, 1 - core, at], dst_ref=pairs.at[sec, at],
            send_sem=ps.at[sec], recv_sem=pr.at[sec, which],
            device_id=(s, partner), device_id_type=MESH)

    def piece_of(p):
        return pl.ds(p * sub, sub)

    def grad_copy(sec, to, p):
        return pltpu.make_async_remote_copy(
            src_ref=gsend.at[sec, core, to, piece_of(p)], dst_ref=recv1.at[sec, chip, piece_of(p)],
            send_sem=gs.at[sec], recv_sem=gr.at[sec, p],
            device_id=(s, 2 * to + core), device_id_type=MESH)

    def sum_copy(sec, p):
        return pltpu.make_async_remote_copy(
            src_ref=zsend.at[sec, piece_of(p)], dst_ref=recv2.at[s, piece_of(p)],
            send_sem=us, recv_sem=ur.at[p],
            device_id=(sec, d), device_id_type=MESH)

    def wgrad(sec, which):
        rounded = ds[1 if which else 0].reshape(M, C)
        shifted(1, rounded, False)
        act = kept[sec, which]
        for a in range(3):
            block = lax.dot_general(
                act, pads[1, :, 2 - a : 2 - a + H].reshape(M, 3 * C),
                (((0,), (0,)), ((), ())), preferred_element_type=jnp.float32)
            for b in range(3):
                g32[(3 * a + b) * C : (3 * a + b + 1) * C] = block[:, b * C : (b + 1) * C]

        def convert(parity):
            for i in range(HC):
                at = 2 * i + parity
                gsend[sec, parity, which * HC + i] = g32[
                    pl.ds(pl.multiple_of(at * rows, 8), rows)].astype(jnp.bfloat16)

        convert(1 - core)
        pair_copy(sec, which).start()
        convert(core)

    def dgrad(sec, which):
        total = jnp.zeros((M, C), jnp.float32)
        for a in range(3):
            for b in range(3):
                tap = 3 * a + b
                total += lax.dot_general(
                    pads[1, :, 2 - a : 2 - a + H, :, b * C : (b + 1) * C].reshape(M, C),
                    wbuf[sec, which * 9 * C + tap * C : which * 9 * C + (tap + 1) * C],
                    (((1,), (1,)), ((), ())), preferred_element_type=jnp.float32)
        into = 0 if which else 1
        ds[into] = ds[into] + (total * slopes[sec, which]).reshape(share, H, W, C)

    def combine(sec, which):
        pair_copy(sec, which).wait_recv()
        for i in range(HC):
            to = which * HC + i
            both = gsend[sec, core, to].astype(jnp.float32) + pairs[sec, to].astype(jnp.float32)
            gsend[sec, core, to] = both.astype(jnp.bfloat16)

            @pl.when(to != chip)
            def _():
                for p in range(NP):
                    grad_copy(sec, to, p).start()

    def finish(sec, p):
        all_of(recv1.at[sec, pl.ds(0, chips - 1), piece_of(p)], gs.at[sec], gr.at[sec, p]).wait_recv()

        def add(i, total):
            return total + recv1[sec, other_chip(i), piece_of(p)].astype(jnp.float32)

        total = lax.fori_loop(
            1, chips, add, gsend[sec, core, chip, piece_of(p)].astype(jnp.float32))

        @pl.when(sec == s)
        def _():
            gown[piece_of(p)] = total

        @pl.when(sec != s)
        def _():
            zsend[sec, piece_of(p)] = total.astype(jnp.bfloat16)
            sum_copy(sec, p).start()

    def backward_one(turn, carry):
        sec = S - 1 - turn
        with scope("b_wg"):
            wgrad(sec, 1)

        with scope("b_comb"):
            @pl.when(turn > 0)
            def _():
                combine(sec + 1, 0)

        with scope("b_dg"):
            dgrad(sec, 1)
        with scope("b_wg"):
            wgrad(sec, 0)
        with scope("b_comb"):
            combine(sec, 1)

        @pl.when(turn < S - 1)
        def _():
            with scope("b_dg"):
                dgrad(sec, 0)

            @pl.when(turn > 1)
            def _():
                with scope("b_fin"):
                    for p in range(NP):
                        finish(sec + 2, p)

        return carry

    lax.fori_loop(0, S, backward_one, 0)
    with scope("c_comb"):
        combine(0, 0)
    with scope("c_fin1"):
        for sec in range(min(S, 3) - 1, 0, -1):
            for p in range(NP):
                finish(sec, p)
    with scope("c_fin0"):
        for p in range(NP):
            finish(0, p)

    def out_copy(to, p):
        return pltpu.make_async_remote_copy(
            src_ref=new_weights.at[d, piece_of(p)], dst_ref=new_weights.at[d, piece_of(p)],
            send_sem=os, recv_sem=orr.at[p],
            device_id=(s, 2 * to + core), device_id_type=MESH)

    def hand_over(src, p):
        return pltpu.make_async_remote_copy(
            src_ref=new_weights.at[src, piece_of(p)], dst_ref=new_weights.at[src, piece_of(p)],
            send_sem=fs, recv_sem=fr,
            device_id=(s, partner), device_id_type=MESH)

    for p in range(NP):
        with scope("c_sum"):
            all_of(recv2.at[pl.ds(0, S - 1), piece_of(p)], us, ur.at[p]).wait_recv()
        with scope("c_upd"):
            def gather_sums(i, total):
                return total + recv2[lax.rem(s + i, S), piece_of(p)].astype(jnp.float32)

            summed = lax.fori_loop(1, S, gather_sums, gown[piece_of(p)])
            moved = inertia * old_momentum[piece_of(p)] + summed / images
            new_momentum[piece_of(p)] = moved
            fresh = old_master[piece_of(p)] - step_size * moved
            new_master[piece_of(p)] = fresh
            new_weights[d, piece_of(p)] = fresh.astype(jnp.bfloat16)

            @pl.loop(1, chips)
            def _(i):
                out_copy(other_chip(i), p).start()

            hand_over(d, p).start()

    with scope("c_sent"):
        @pl.when(sends)
        def _():
            all_of(wbuf.at[0, pl.ds(0, 2 * (S - 1) * piece)], zs, zr.at[0, 0]).wait_send()

        @pl.loop(0, S)
        def _(sec):
            @pl.when(sec != s)
            def _():
                @pl.when(sends)
                def _():
                    for h in range(2):
                        all_of(wbuf.at[sec, pl.ds(0, (chips - 1) * piece)], ls.at[sec, h], lr.at[sec, h]).wait_send()

                all_of(wbuf.at[sec, pl.ds(0, 2 * CK * piece)], cs.at[sec], cr.at[sec, 0]).wait_send()

            all_of(gsend.at[sec, 0], ps.at[sec], pr.at[sec, 0]).wait_send()
            all_of(recv1.at[sec, pl.ds(0, chips - 1)], gs.at[sec], gr.at[sec, 0]).wait_send()

        all_of(recv2.at[pl.ds(0, S - 1)], us, ur.at[0]).wait_send()

    for p in range(NP):
        with scope("c_orecv"):
            all_of(recv1.at[0, pl.ds(0, chips - 1), piece_of(p)], os, orr.at[p]).wait_recv()

        @pl.loop(1, chips)
        def _(i):
            hand_over(2 * other_chip(i) + core, p).start()

    with scope("c_end"):
        all_of(recv1.at[0, pl.ds(0, chips - 1)], os, orr.at[0]).wait_send()
        all_of(recv1.at[0], fs, fr).wait_send()
        all_of(recv1.at[0], fs, fr).wait_recv()


def store(a, b, c, out_a, out_b, out_c, sem):
    copies = [
        pltpu.make_async_copy(c, out_c, sem.at[2]),
        pltpu.make_async_copy(a, out_a, sem.at[0]),
        pltpu.make_async_copy(b, out_b, sem.at[1]),
    ]
    for copy in copies:
        copy.start()
    for copy in copies:
        copy.wait()


def on_device(S, D, stream, cotangent, weights, master, momentum):
    _, per_dp, H, W, C = stream.shape
    share = per_dp // S
    M = share * H * W
    R = weights.shape[1]
    rows = master.shape[1]
    chips = D // 2
    NP = 3 if rows % 48 == 0 else 1
    bf, f32 = jnp.bfloat16, jnp.float32
    vmem = pl.BlockSpec(memory_space=pltpu.VMEM)
    hbm = pl.BlockSpec(memory_space=pltpu.HBM)
    dma = pltpu.SemaphoreType.DMA
    results = pl.pallas_call(
        functools.partial(kernel, S, D, per_dp * D, NP),
        out_shape=(
            pltpu.VMEM((rows, C), f32),
            pltpu.VMEM((rows, C), f32),
            pltpu.VMEM((D, rows, C), bf),
        ),
        in_specs=[hbm] * 5,
        out_specs=(vmem, vmem, vmem),
        scratch_shapes=[
            pltpu.VMEM((S, R, C), bf),
            pltpu.VMEM((2, share, H, W, C), f32),
            pltpu.VMEM((2, share, H, W, C), f32),
            pltpu.VMEM((2, share, H + 2, W, 3 * C), bf),
            pltpu.VMEM((S, 2, M, C), bf),
            pltpu.VMEM((S, 2, M, C), f32),
            pltpu.VMEM((R // 2, C), f32),
            pltpu.VMEM((S, 2, chips, rows, C), bf),
            pltpu.VMEM((S, chips, rows, C), bf),
            pltpu.VMEM((S, chips, rows, C), bf),
            pltpu.VMEM((S, rows, C), bf),
            pltpu.VMEM((S, rows, C), bf),
            pltpu.VMEM((rows, C), f32),
            pltpu.VMEM((rows, C), f32),
            pltpu.VMEM((rows, C), f32),
            dma((7,)), dma, dma((S, 2)), dma((S, 2)), dma((S, 2)), dma((S,)), dma((S, 2)),
            dma((S,)), dma((S, 2)), dma((S,)), dma((S, NP)), dma, dma((NP,)),
            dma, dma((NP,)), dma, dma,
        ],
        compiler_params=pltpu.CompilerParams(
            has_side_effects=True, collective_id=0, vmem_limit_bytes=48 * 1024 * 1024),
    )(*[pltpu.with_memory_space_constraint(x, pltpu.HBM)
        for x in (stream, cotangent, weights[0], master[0], momentum[0])])
    new_master, new_momentum, new_weights = pl.pallas_call(
        store,
        out_shape=(
            jax.ShapeDtypeStruct((rows, C), f32),
            jax.ShapeDtypeStruct((rows, C), f32),
            jax.ShapeDtypeStruct((D, rows, C), bf),
        ),
        in_specs=[vmem] * 3,
        out_specs=(hbm, hbm, hbm),
        scratch_shapes=[dma((3,))],
        compiler_params=pltpu.CompilerParams(vmem_limit_bytes=4 * 1024 * 1024),
    )(*[pltpu.with_memory_space_constraint(x, pltpu.VMEM) for x in results])
    return (new_master[None], new_momentum[None], new_weights.reshape(1, R, C))


def solution(mesh):
    placed = (
        P(None, "dp", None, None, None),
        P(None, "dp", None, None, None),
        P("section", None, None),
        P("section", "dp", None),
        P("section", "dp", None),
    )
    return jax.shard_map(
        functools.partial(on_device, mesh.shape["section"], mesh.shape["dp"]),
        mesh=mesh,
        in_specs=placed,
        out_specs=(P("section", "dp", None), P("section", "dp", None), P("section", None, None)),
        check_vma=False,
    )
```

```python
import functools
import math

import jax
import jax.numpy as jnp
from jax import lax
from jax.experimental import pallas as pl
from jax.experimental.pallas import tpu as pltpu
from jax.sharding import PartitionSpec as P

MESH = pl.DeviceIdType.MESH
step_size = 0.1
inertia = 0.9
scope = jax.named_scope


def kernel(
    S, D, images, NP,
    stream, cotangent, weights, master, momentum,
    new_master, new_momentum, new_weights,
    wbuf, xs, ds, patches, turned, slopes, g32, gsend, pairs, recv1, zsend, recv2, recv3, gown,
    old_master, old_momentum,
    in_sem, zs, zr, ls, lr, cs, cr, ps, pr, gs, gr, us, ur, vr, os, orr, fs, fr,
):
    s = lax.axis_index("section")
    d = lax.axis_index("dp")
    core = lax.rem(d, 2)
    chip = lax.div(d, 2)
    partner = d + 1 - 2 * core
    chips = D // 2
    HC = chips // 2
    share, H, W, C = xs.shape[1:]
    M = share * H * W
    rows = master.shape[0]
    sub = rows // NP
    R = rows * D
    half = R // 2
    NC = math.gcd(half // 16, D)
    CK = NC // 2
    piece = half // NC
    sends = chip < CK
    square = chips == 4
    across = chip + 1 - 2 * lax.rem(chip, 2)
    along = lax.rem(chip + HC, chips)
    near = across + core * (along - across)
    far = along + core * (across - along)

    def other_chip(i):
        return lax.rem(chip + i, chips)

    def own_piece(h):
        return pl.ds(pl.multiple_of(h * half + (core * CK + chip) * piece, 16), piece)

    def section_copy(sec, h, to):
        return pltpu.make_async_remote_copy(
            src_ref=weights.at[own_piece(h)], dst_ref=wbuf.at[sec, own_piece(h)],
            send_sem=zs, recv_sem=zr.at[sec, h],
            device_id=(to, d), device_id_type=MESH)

    def layer_copy(sec, h, to):
        return pltpu.make_async_remote_copy(
            src_ref=wbuf.at[sec, own_piece(h)], dst_ref=wbuf.at[sec, own_piece(h)],
            send_sem=ls.at[sec, h], recv_sem=lr.at[sec, h],
            device_id=(s, 2 * to + core), device_id_type=MESH)

    def core_copy(sec, h):
        at = pl.ds(pl.multiple_of(h * half + core * (CK * piece), 16), CK * piece)
        return pltpu.make_async_remote_copy(
            src_ref=wbuf.at[sec, at], dst_ref=wbuf.at[sec, at],
            send_sem=cs.at[sec], recv_sem=cr.at[sec, h],
            device_id=(s, partner), device_id_type=MESH)

    def all_of(ref, send_sem, recv_sem):
        return pltpu.make_async_remote_copy(
            src_ref=ref, dst_ref=ref, send_sem=send_sem, recv_sem=recv_sem,
            device_id=(s, partner), device_id_type=MESH)

    def send_down():
        for h in range(2):
            for to in range(S - 1):
                @pl.when(sends & (to < s))
                def _():
                    section_copy(s, h, to).start()

    def send_top(h):
        @pl.when(sends & (s < S - 1))
        def _():
            section_copy(s, h, S - 1).start()

    def send_up(h):
        for to in range(S - 2, 0, -1):
            @pl.when(sends & (to > s))
            def _():
                section_copy(s, h, to).start()

    def relay(sec, h):
        @pl.when((sec != s) & (sec < S) & sends)
        def _():
            section_copy(sec, h, s).wait_recv()

            @pl.loop(1, chips)
            def _(i):
                layer_copy(sec, h, other_chip(i)).start()

    def pass_on(sec, h):
        @pl.when((sec != s) & (sec < S))
        def _():
            @pl.when(sends)
            def _():
                all_of(wbuf.at[sec, pl.ds(0, (CK - 1) * piece)], ls.at[sec, h], lr.at[sec, h]).wait_recv()

            if CK < chips:
                @pl.when(chip >= CK)
                def _():
                    all_of(wbuf.at[sec, pl.ds(0, CK * piece)], ls.at[sec, h], lr.at[sec, h]).wait_recv()

            core_copy(sec, h).start()

    def take(sec, h):
        @pl.when(sec != s)
        def _():
            core_copy(sec, h).wait_recv()

    barrier = pltpu.get_barrier_semaphore()

    @pl.loop(1, S)
    def _(i):
        pl.semaphore_signal(barrier, inc=1, device_id=(lax.rem(s + i, S), d), device_id_type=MESH)

    @pl.loop(1, D)
    def _(i):
        pl.semaphore_signal(barrier, inc=1, device_id=(s, lax.rem(d + i, D)), device_id_type=MESH)

    mine = pl.ds(s * share, share)
    loads = [
        pltpu.make_async_copy(stream.at[1, mine], xs.at[1], in_sem.at[1]),
        pltpu.make_async_copy(stream.at[0, mine], xs.at[0], in_sem.at[0]),
        pltpu.make_async_copy(weights, wbuf.at[s], in_sem.at[6]),
        pltpu.make_async_copy(cotangent.at[0, mine], ds.at[0], in_sem.at[2]),
        pltpu.make_async_copy(cotangent.at[1, mine], ds.at[1], in_sem.at[3]),
        pltpu.make_async_copy(momentum, old_momentum, in_sem.at[4]),
        pltpu.make_async_copy(master, old_master, in_sem.at[5]),
    ]
    for load in loads:
        load.start()

    with scope("t_bar"):
        pl.semaphore_wait(barrier, S + D - 2)
    send_top(0)
    send_down()

    @pl.when(s == 0)
    def _():
        send_up(0)
        send_top(1)
        send_up(1)

    col = lax.rem(lax.broadcasted_iota(jnp.int32, (M, C), 0), W)

    def column_taps(flat):
        before = jnp.where(col == 0, 0.0, pltpu.roll(flat, 1, 0))
        after = jnp.where(col == W - 1, 0.0, pltpu.roll(flat, M - 1, 0))
        return [x.astype(jnp.bfloat16) for x in (before, flat, after)]

    def row_moved(flat, by):
        if by == 0:
            return flat
        field = flat.reshape(share, H, W, C)
        edge = jnp.zeros((share, 1, W, C), flat.dtype)
        parts = (edge, field[:, : H - 1]) if by > 0 else (field[:, 1:], edge)
        return jnp.concatenate(parts, axis=1).reshape(M, C)

    def activate(value, sec, which):
        logistic = 1.0 / (1.0 + jnp.exp(-value))
        act = value * logistic
        slopes[sec, which] = logistic * (1.0 + value * (1.0 - logistic))
        for b, tap in enumerate(column_taps(act)):
            patches[:, b * C : (b + 1) * C] = tap
            turned[sec, which, b * C : (b + 1) * C] = tap.T

    def conv(sec, which):
        wide = jnp.concatenate(
            [wbuf[sec, which * 9 * C + a * 3 * C : which * 9 * C + (a + 1) * 3 * C] for a in range(3)],
            axis=1)
        found = jnp.dot(patches[...], wide, preferred_element_type=jnp.float32)
        return sum(row_moved(found[:, a * C : (a + 1) * C], 1 - a) for a in range(3))

    with scope("t_load"):
        for load in loads[:3]:
            load.wait()
    with scope("t_act"):
        activate(xs[1].reshape(M, C), 0, 0)
    with scope("t_rel"):
        relay(0, 0)

        @pl.when(s > 0)
        def _():
            send_top(1)
            send_up(0)
            send_up(1)

        relay(0, 1)
        relay(1, 0)
    with scope("t_pass"):
        pass_on(0, 0)

    def forward_one(sec, carry):
        with scope("t_rel"):
            relay(sec + 1, 1)
        with scope("t_take"):
            take(sec, 0)

        @pl.when(sec > 0)
        def _():
            with scope("t_pass"):
                pass_on(sec, 1)

        with scope("t_conv"):
            first = xs[0].reshape(M, C) + conv(sec, 0)
        with scope("t_act"):
            activate(first, sec, 1)
            xs[0] = first.reshape(share, H, W, C)

        @pl.when(sec == 0)
        def _():
            with scope("t_pass"):
                pass_on(sec, 1)

        with scope("t_rel"):
            relay(sec + 2, 0)
        with scope("t_take"):
            take(sec, 1)
        with scope("t_pass"):
            pass_on(sec + 1, 0)
        with scope("t_conv"):
            second = xs[1].reshape(M, C) + conv(sec, 1)

        @pl.when(sec + 1 < S)
        def _():
            with scope("t_act"):
                activate(second, sec + 1, 0)
                xs[1] = second.reshape(share, H, W, C)

        return carry

    lax.fori_loop(0, S, forward_one, 0)
    for load in loads[3:]:
        load.wait()

    def pair_copy(sec, which):
        at = pl.ds(which * HC, HC)
        return pltpu.make_async_remote_copy(
            src_ref=gsend.at[sec, 1 - core, at], dst_ref=pairs.at[sec, at],
            send_sem=ps.at[sec], recv_sem=pr.at[sec, which],
            device_id=(s, partner), device_id_type=MESH)

    def piece_of(p):
        return pl.ds(p * sub, sub)

    def grad_copy(sec, to, p):
        return pltpu.make_async_remote_copy(
            src_ref=gsend.at[sec, core, to, piece_of(p)], dst_ref=recv1.at[sec, chip, piece_of(p)],
            send_sem=gs.at[sec], recv_sem=gr.at[sec, p],
            device_id=(s, 2 * to + core), device_id_type=MESH)

    def near_copy(sec, piece_, slot):
        return pltpu.make_async_remote_copy(
            src_ref=gsend.at[sec, core, piece_], dst_ref=recv1.at[sec, slot],
            send_sem=gs.at[sec], recv_sem=gr.at[sec, 0],
            device_id=(s, 2 * near + core), device_id_type=MESH)

    def far_copy(sec):
        return pltpu.make_async_remote_copy(
            src_ref=gsend.at[sec, core, far], dst_ref=recv1.at[sec, 2],
            send_sem=gs.at[sec], recv_sem=gr.at[sec, 1],
            device_id=(s, 2 * far + core), device_id_type=MESH)

    def sum_copy(sec, p):
        return pltpu.make_async_remote_copy(
            src_ref=zsend.at[sec, piece_of(p)], dst_ref=recv2.at[s, piece_of(p)],
            send_sem=us, recv_sem=ur.at[p],
            device_id=(sec, d), device_id_type=MESH)

    def step_copy(p):
        return pltpu.make_async_remote_copy(
            src_ref=zsend.at[0, piece_of(p)], dst_ref=recv3.at[piece_of(p)],
            send_sem=us, recv_sem=vr.at[p],
            device_id=(s - 1, d), device_id_type=MESH)

    def wgrad(sec, which):
        rounded = ds[1 if which else 0].reshape(M, C).astype(jnp.bfloat16)
        moved = jnp.concatenate([row_moved(rounded, a - 1) for a in range(3)], axis=1)
        found = jnp.dot(turned[sec, which], moved, preferred_element_type=jnp.float32)
        for a in range(3):
            for b in range(3):
                g32[(3 * a + b) * C : (3 * a + b + 1) * C] = found[
                    b * C : (b + 1) * C, a * C : (a + 1) * C]

        def convert(parity):
            for i in range(HC):
                at = 2 * i + parity
                gsend[sec, parity, which * HC + i] = g32[
                    pl.ds(pl.multiple_of(at * rows, 8), rows)].astype(jnp.bfloat16)

        convert(1 - core)
        pair_copy(sec, which).start()
        convert(core)

    def dgrad(sec, which):
        before, at, after = column_taps(ds[1 if which else 0].reshape(M, C))
        wide = jnp.concatenate([after, at, before], axis=1)
        taps = wbuf[sec, which * 9 * C : (which + 1) * 9 * C].reshape(3, 3, C, C)
        turn = jnp.concatenate(
            [jnp.concatenate([taps[a, b] for b in range(3)], axis=1) for a in range(3)], axis=0)
        found = lax.dot_general(
            wide, turn, (((1,), (1,)), ((), ())), preferred_element_type=jnp.float32)
        total = sum(row_moved(found[:, a * C : (a + 1) * C], a - 1) for a in range(3))
        into = 0 if which else 1
        ds[into] = ds[into] + (total * slopes[sec, which]).reshape(share, H, W, C)

    def combine(sec, which):
        direct = sec == 0 if square else True
        pair_copy(sec, which).wait_recv()
        for i in range(HC):
            to = which * HC + i
            both = gsend[sec, core, to].astype(jnp.float32) + pairs[sec, to].astype(jnp.float32)
            gsend[sec, core, to] = both.astype(jnp.bfloat16)

            @pl.when((to != chip) & direct)
            def _():
                for p in range(NP):
                    grad_copy(sec, to, p).start()

            if square:
                @pl.when((to == near) & (sec != 0))
                def _():
                    near_copy(sec, to, 0).start()

                @pl.when((to == chips - 1 - chip) & (sec != 0))
                def _():
                    near_copy(sec, to, 1).start()

    def step(sec):
        if square:
            all_of(recv1.at[sec, pl.ds(0, 2)], gs.at[sec], gr.at[sec, 0]).wait_recv()
            both = gsend[sec, core, far].astype(jnp.float32) + recv1[sec, 1].astype(jnp.float32)
            gsend[sec, core, far] = both.astype(jnp.bfloat16)
            far_copy(sec).start()

    def hand_in(sec, p, total):
        @pl.when(sec == s)
        def _():
            gown[piece_of(p)] = total

        @pl.when(sec != s)
        def _():
            zsend[sec, piece_of(p)] = total.astype(jnp.bfloat16)
            sum_copy(sec, p).start()

    def plane_sum(sec, p):
        all_of(recv1.at[sec, pl.ds(0, chips - 1), piece_of(p)], gs.at[sec], gr.at[sec, p]).wait_recv()

        def add(i, total):
            return total + recv1[sec, other_chip(i), piece_of(p)].astype(jnp.float32)

        return lax.fori_loop(
            1, chips, add, gsend[sec, core, chip, piece_of(p)].astype(jnp.float32))

    def finish(sec):
        if square:
            all_of(recv1.at[sec, 2], gs.at[sec], gr.at[sec, 1]).wait_recv()
        for p in range(NP):
            if square:
                total = sum(
                    ref[piece_of(p)].astype(jnp.float32)
                    for ref in (gsend.at[sec, core, chip], recv1.at[sec, 0], recv1.at[sec, 2]))
            else:
                total = plane_sum(sec, p)
            hand_in(sec, p, total)

    def finish_last(p):
        total = plane_sum(0, p)

        @pl.when(s == 0)
        def _():
            gown[piece_of(p)] = total

        @pl.when((s > 1) & (lax.rem(s, 2) == 1))
        def _():
            zsend[0, piece_of(p)] = total.astype(jnp.bfloat16)
            step_copy(p).start()

        @pl.when((s == 1) | ((s == S - 1) & (lax.rem(s, 2) == 0)))
        def _():
            zsend[0, piece_of(p)] = total.astype(jnp.bfloat16)
            sum_copy(0, p).start()

        @pl.when((s > 0) & (s < S - 1) & (lax.rem(s, 2) == 0))
        def _():
            step_copy(p).wait_recv()
            zsend[0, piece_of(p)] = (total + recv3[piece_of(p)].astype(jnp.float32)).astype(jnp.bfloat16)
            sum_copy(0, p).start()

    def backward_one(turn, carry):
        sec = S - 1 - turn
        with scope("b_wg"):
            wgrad(sec, 1)

        with scope("b_comb"):
            @pl.when(turn > 0)
            def _():
                combine(sec + 1, 0)

        with scope("b_dg"):
            dgrad(sec, 1)
        with scope("b_wg"):
            wgrad(sec, 0)
        with scope("b_comb"):
            combine(sec, 1)

        @pl.when(turn < S - 1)
        def _():
            with scope("b_dg"):
                dgrad(sec, 0)

        @pl.when(turn > 1)
        def _():
            with scope("b_step"):
                step(sec + 2)

        @pl.when(turn > 3)
        def _():
            with scope("b_fin"):
                finish(sec + 4)

        return carry

    lax.fori_loop(0, S, backward_one, 0)
    with scope("c_comb"):
        combine(0, 0)
    with scope("c_step"):
        if S > 1:
            step(1)
    with scope("c_fin1"):
        for sec in range(min(S, 4) - 1, 1, -1):
            finish(sec)
    with scope("c_fin0"):
        for p in range(NP):
            finish_last(p)
    with scope("c_fin2"):
        if S > 1:
            finish(1)

    def out_copy(to, p):
        return pltpu.make_async_remote_copy(
            src_ref=new_weights.at[d, piece_of(p)], dst_ref=new_weights.at[d, piece_of(p)],
            send_sem=os, recv_sem=orr.at[p],
            device_id=(s, 2 * to + core), device_id_type=MESH)

    def hand_over(src, p):
        return pltpu.make_async_remote_copy(
            src_ref=new_weights.at[src, piece_of(p)], dst_ref=new_weights.at[src, piece_of(p)],
            send_sem=fs, recv_sem=fr,
            device_id=(s, partner), device_id_type=MESH)

    few = 1 + (S - 1) // 2
    parts = jnp.where(s == 0, few, S - 1)

    def part(i):
        return jnp.where(s == 0, jnp.maximum(2 * i, 1), lax.rem(s + i + 1, S))

    for p in range(NP):
        with scope("c_sum"):
            @pl.when(s == 0)
            def _():
                all_of(recv2.at[pl.ds(0, few), piece_of(p)], us, ur.at[p]).wait_recv()

            @pl.when(s != 0)
            def _():
                all_of(recv2.at[pl.ds(0, S - 1), piece_of(p)], us, ur.at[p]).wait_recv()
        with scope("c_upd"):
            def gather_sums(i, total):
                return total + recv2[part(i), piece_of(p)].astype(jnp.float32)

            summed = lax.fori_loop(0, parts, gather_sums, gown[piece_of(p)])
            moved = inertia * old_momentum[piece_of(p)] + summed / images
            new_momentum[piece_of(p)] = moved
            fresh = old_master[piece_of(p)] - step_size * moved
            new_master[piece_of(p)] = fresh
            new_weights[d, piece_of(p)] = fresh.astype(jnp.bfloat16)

            @pl.loop(1, chips)
            def _(i):
                out_copy(other_chip(i), p).start()

            hand_over(d, p).start()

    with scope("c_sent"):
        @pl.when(sends)
        def _():
            all_of(wbuf.at[0, pl.ds(0, 2 * (S - 1) * piece)], zs, zr.at[0, 0]).wait_send()

        @pl.loop(0, S)
        def _(sec):
            @pl.when(sec != s)
            def _():
                @pl.when(sends)
                def _():
                    for h in range(2):
                        all_of(wbuf.at[sec, pl.ds(0, (chips - 1) * piece)], ls.at[sec, h], lr.at[sec, h]).wait_send()

                all_of(wbuf.at[sec, pl.ds(0, 2 * CK * piece)], cs.at[sec], cr.at[sec, 0]).wait_send()

            all_of(gsend.at[sec, 0], ps.at[sec], pr.at[sec, 0]).wait_send()
            all_of(recv1.at[sec, pl.ds(0, chips - 1)], gs.at[sec], gr.at[sec, 0]).wait_send()

        all_of(recv2.at[pl.ds(0, S - 1)], us, ur.at[0]).wait_send()

    for p in range(NP):
        with scope("c_orecv"):
            all_of(recv1.at[0, pl.ds(0, chips - 1), piece_of(p)], os, orr.at[p]).wait_recv()

        @pl.loop(1, chips)
        def _(i):
            hand_over(2 * other_chip(i) + core, p).start()

    with scope("c_end"):
        all_of(recv1.at[0, pl.ds(0, chips - 1)], os, orr.at[0]).wait_send()
        all_of(recv1.at[0], fs, fr).wait_send()
        all_of(recv1.at[0], fs, fr).wait_recv()


def store(a, b, c, out_a, out_b, out_c, sem):
    copies = [
        pltpu.make_async_copy(c, out_c, sem.at[2]),
        pltpu.make_async_copy(a, out_a, sem.at[0]),
        pltpu.make_async_copy(b, out_b, sem.at[1]),
    ]
    for copy in copies:
        copy.start()
    for copy in copies:
        copy.wait()


def on_device(S, D, stream, cotangent, weights, master, momentum):
    _, per_dp, H, W, C = stream.shape
    share = per_dp // S
    M = share * H * W
    R = weights.shape[1]
    rows = master.shape[1]
    chips = D // 2
    NP = 3 if rows % 48 == 0 else 1
    bf, f32 = jnp.bfloat16, jnp.float32
    vmem = pl.BlockSpec(memory_space=pltpu.VMEM)
    hbm = pl.BlockSpec(memory_space=pltpu.HBM)
    dma = pltpu.SemaphoreType.DMA
    results = pl.pallas_call(
        functools.partial(kernel, S, D, per_dp * D, NP),
        out_shape=(
            pltpu.VMEM((rows, C), f32),
            pltpu.VMEM((rows, C), f32),
            pltpu.VMEM((D, rows, C), bf),
        ),
        in_specs=[hbm] * 5,
        out_specs=(vmem, vmem, vmem),
        scratch_shapes=[
            pltpu.VMEM((S, R, C), bf),
            pltpu.VMEM((2, share, H, W, C), f32),
            pltpu.VMEM((2, share, H, W, C), f32),
            pltpu.VMEM((M, 3 * C), bf),
            pltpu.VMEM((S, 2, 3 * C, M), bf),
            pltpu.VMEM((S, 2, M, C), f32),
            pltpu.VMEM((R // 2, C), f32),
            pltpu.VMEM((S, 2, chips, rows, C), bf),
            pltpu.VMEM((S, chips, rows, C), bf),
            pltpu.VMEM((S, chips, rows, C), bf),
            pltpu.VMEM((S, rows, C), bf),
            pltpu.VMEM((S, rows, C), bf),
            pltpu.VMEM((rows, C), bf),
            pltpu.VMEM((rows, C), f32),
            pltpu.VMEM((rows, C), f32),
            pltpu.VMEM((rows, C), f32),
            dma((7,)), dma, dma((S, 2)), dma((S, 2)), dma((S, 2)), dma((S,)), dma((S, 2)),
            dma((S,)), dma((S, 2)), dma((S,)), dma((S, max(NP, 2))), dma, dma((NP,)), dma((NP,)),
            dma, dma((NP,)), dma, dma,
        ],
        compiler_params=pltpu.CompilerParams(
            has_side_effects=True, collective_id=0, vmem_limit_bytes=48 * 1024 * 1024),
    )(*[pltpu.with_memory_space_constraint(x, pltpu.HBM)
        for x in (stream, cotangent, weights[0], master[0], momentum[0])])
    new_master, new_momentum, new_weights = pl.pallas_call(
        store,
        out_shape=(
            jax.ShapeDtypeStruct((rows, C), f32),
            jax.ShapeDtypeStruct((rows, C), f32),
            jax.ShapeDtypeStruct((D, rows, C), bf),
        ),
        in_specs=[vmem] * 3,
        out_specs=(hbm, hbm, hbm),
        scratch_shapes=[dma((3,))],
        compiler_params=pltpu.CompilerParams(vmem_limit_bytes=4 * 1024 * 1024),
    )(*[pltpu.with_memory_space_constraint(x, pltpu.VMEM) for x in results])
    return (new_master[None], new_momentum[None], new_weights.reshape(1, R, C))


def solution(mesh):
    placed = (
        P(None, "dp", None, None, None),
        P(None, "dp", None, None, None),
        P("section", None, None),
        P("section", "dp", None),
        P("section", "dp", None),
    )
    return jax.shard_map(
        functools.partial(on_device, mesh.shape["section"], mesh.shape["dp"]),
        mesh=mesh,
        in_specs=placed,
        out_specs=(P("section", "dp", None), P("section", "dp", None), P("section", None, None)),
        check_vma=False,
    )
```
